32 devices in a mesh: owner: 4 (over z), slab: 2 (over y), red: 4 (over x, core).
Axes of the slice: x: 2, y: 2, z: 4, core: 2. Of those that a mesh axis runs over, the one named last changes fastest.
Arguments:
- amplitudes: bfloat16 [64, 128, 256], P(('owner', 'slab', 'red')), may hold values from -6 to 6
- integrals: bfloat16 [32, 128, 128], P('slab'), may hold values from -0.21875 to 0.21875
- requests: int32 [4, 2, 4, 4], P('owner', 'slab', 'red'), may hold values from 0 to 1
- task_slot: int32 [4, 2, 4, 8, 12], P('owner', 'slab', 'red'), may hold values from 0 to 3
- task_integral: int32 [4, 2, 4, 8, 12], P('owner', 'slab', 'red'), may hold values from 0 to 31
- live_tasks: int32 [4, 2, 4], P('owner', 'slab', 'red'), may hold values from 3 to 12, as said below
- denominators: float32 [64, 128, 256], P(('owner', 'slab', 'red')), may hold values from 0.5 to 5
Outputs:
- update: float32 [64, 128, 256], P(('owner', 'slab', 'red'))
The draws below stay inside these ranges and needn't reach their ends.
Inputs may be any that keep to these rules, and one draw needn't show every extreme that they name: `live_tasks`: slots below a device's count are live; in every draw some devices have all 12 live.
All inputs are finite; a program needn't handle non-finite values.
Results may differ from the reference program's by a relative error of at most 0.0003.
Values may be sent and summed in bfloat16 or wider, within the bound.
A program may use at most 64 MiB of HBM per device.

```python
import math
import jax
import jax.numpy as jnp
from jax import lax

TILE = 128
COLUMNS = 256
OWNED = 2
SLOTS = 12
AMP_TILES = 64
INT_TILES = 32
GROUP_OUT = 8
OUT_TOTAL = 64
N_OWNER = 4
N_SLAB = 2
N_RED = 4


def draw_live_tasks(key, part):
    base_key = jax.random.fold_in(key, 7)
    first_key, second_key = jax.random.split(base_key)
    devices_all = N_OWNER * N_SLAB * N_RED
    base = jax.random.randint(first_key, (devices_all,), SLOTS // 4, SLOTS // 2 + 1, dtype=jnp.int32)
    order = jax.random.permutation(second_key, devices_all)
    heavy = order < max(devices_all // 16, 1)
    filled = jnp.where(heavy, SLOTS, base).astype(jnp.int32)
    return filled.reshape(N_OWNER, N_SLAB, N_RED)


def touch_ends(values, stream_key, low, top_value):
    extent = values.shape
    index_at = [jax.random.randint(jax.random.fold_in(stream_key, axis), (), 0, extent[axis]) for axis in range(len(extent))]
    values = values.at[tuple(index_at)].set(low)
    longest = extent.index(max(extent))
    index_at[longest] = (index_at[longest] + 1) % extent[longest]
    return values.at[tuple(index_at)].set(top_value)


def level_of(key, extent, cuts, low, high):
    def one(dim, parts):
        steps = jax.random.uniform(jax.random.fold_in(jax.random.fold_in(key, 6), dim), (parts,), jnp.float32, low / len(cuts), high / len(cuts))
        return jnp.repeat(jnp.exp(steps), extent[dim] // parts).reshape((-1,) + (1,) * (len(extent) - dim - 1))

    factor_of = one(*cuts[0])
    for cut in cuts[1:]:
        factor_of = factor_of * one(*cut)
    return factor_of


def gaussian(own_key, shape, scale, bound, cuts=(), kind=jnp.bfloat16):
    drawn = jax.random.normal(own_key, shape, jnp.float32) * scale
    if len(cuts) > 0:
        drawn = level_of(own_key, shape, cuts, -0.22, 0.18) * drawn
    return jnp.clip(drawn, min=-bound, max=bound).astype(kind)


def setup_inputs(seed: int = 0) -> dict:
    arg_keys = jax.random.split(jax.random.key(seed), 8)
    return {
        "amplitudes": gaussian(arg_keys[0], (AMP_TILES, TILE, COLUMNS), 1.0, 6.0, ((0, 32),)),
        "integrals": gaussian(arg_keys[1], (INT_TILES, TILE, TILE), (TILE * SLOTS // 2) ** -0.5, 0.21875, ((0, 2),)),
        "requests": touch_ends(jax.random.randint(arg_keys[2], (N_OWNER, N_SLAB, N_RED, N_OWNER), 0, OWNED), jax.random.fold_in(arg_keys[2], 1), 0, OWNED - 1).astype(jnp.int32),
        "task_slot": touch_ends(jax.random.randint(arg_keys[3], (N_OWNER, N_SLAB, N_RED, GROUP_OUT, SLOTS), 0, N_OWNER), jax.random.fold_in(arg_keys[3], 1), 0, N_OWNER - 1).astype(jnp.int32),
        "task_integral": touch_ends(jax.random.randint(arg_keys[4], (N_OWNER, N_SLAB, N_RED, GROUP_OUT, SLOTS), 0, INT_TILES), jax.random.fold_in(arg_keys[4], 1), 0, INT_TILES - 1).astype(jnp.int32),
        "live_tasks": draw_live_tasks(jax.random.fold_in(arg_keys[7], 71), 0),
        "denominators": jnp.clip(jnp.exp(math.log(5.0) - 2.3025851 * jax.random.uniform(arg_keys[6], (OUT_TOTAL, TILE, COLUMNS), jnp.float32) ** level_of(arg_keys[6], (OUT_TOTAL, TILE, COLUMNS), ((0, 32),), -0.2, 0.2)), 0.5, 5.0),
    }


def device_partial(column_tiles, integrals, wanted, slot_table, integral_table, live_count):
    pulled = column_tiles[jnp.arange(N_OWNER, dtype=jnp.int32), wanted.astype(jnp.int32)]
    live_mask = (jnp.arange(SLOTS, dtype=jnp.int32) < live_count).astype(jnp.float32)
    integral_rows = integrals[integral_table].astype(jnp.float32) * live_mask[None, :, None, None]
    amplitude_rows = pulled[slot_table].astype(jnp.float32)
    return jnp.einsum("qkac,qkcx->qax", integral_rows, amplitude_rows, precision=lax.Precision.HIGHEST)


def reference(amplitudes, integrals, requests, task_slot, task_integral, live_tasks, denominators):
    groups = N_OWNER * N_SLAB
    blocks = amplitudes.reshape(N_OWNER, N_SLAB, N_RED, OWNED, TILE, COLUMNS)
    per_column = jnp.transpose(blocks, (1, 2, 0, 3, 4, 5))
    request_rows = requests.reshape(groups, N_RED, N_OWNER)
    slot_rows = task_slot.reshape(groups, N_RED, GROUP_OUT, SLOTS)
    integral_ids = task_integral.reshape(groups, N_RED, GROUP_OUT, SLOTS)
    live_rows = live_tasks.reshape(groups, N_RED)
    slab_ids = jnp.tile(jnp.arange(N_SLAB, dtype=jnp.int32), N_OWNER)
    red_ids = jnp.arange(N_RED, dtype=jnp.int32)

    def one_group(bundle):
        slab_index, wanted_rows, slot_group, integral_group, live_group = bundle

        def add_member(summed, member):
            red_index, wanted, slot_table, integral_table, live_count = member
            column_tiles = per_column[slab_index, red_index]
            return summed + device_partial(column_tiles, integrals, wanted, slot_table, integral_table, live_count), None

        initial = jnp.zeros((GROUP_OUT, TILE, COLUMNS), jnp.float32)
        summed, _ = lax.scan(add_member, initial, (red_ids, wanted_rows, slot_group, integral_group, live_group))
        return summed

    sums = lax.map(one_group, (slab_ids, request_rows, slot_rows, integral_ids, live_rows))
    residual = sums.reshape(OUT_TOTAL, TILE, COLUMNS)
    return residual / denominators
```

```python
import functools

import jax
import jax.numpy as jnp
from jax import lax
from jax.experimental import pallas as pl
from jax.experimental.pallas import tpu as pltpu
from jax.sharding import PartitionSpec as P

MESH = pl.DeviceIdType.MESH
CORES = 2
INT_CHUNKS = 2


def kernel(sizes, amp_hbm, int_hbm, req_hbm, slot_hbm, task_hbm, live_hbm, out_ref, *scratch):
    owners, slabs, reds, per_owner, int_local, group_tiles, slots = sizes
    chips = reds // CORES
    keep = group_tiles // reds
    (mine, ints, below, above, stage, own, part) = scratch[:7]
    far = scratch[7 : 7 + 2 * (chips - 1)]
    (req_v, slot_v, task_v, live_v, my_req_s, req_s, slot_s, task_s, live_s,
     local_sem, req_send, req_recv, tab_send, tab_recv, near_send, near_recv, z_send, z_recv,
     int_send, int_recv, intf_send, intf_recv, part_send, part_recv,
     x_send, x_recv, f_send, f_recv) = scratch[7 + 2 * (chips - 1):]
    o = lax.axis_index("owner")
    s = lax.axis_index("slab")
    r = lax.axis_index("red")
    chip = r // CORES
    core = r % CORES
    mate = chip * CORES + (1 - core)

    def rcopy(src, dst, send, recv, **where):
        return pltpu.make_async_remote_copy(
            src_ref=src, dst_ref=dst, send_sem=send, recv_sem=recv, device_id=where, device_id_type=MESH
        )

    local = [
        pltpu.make_async_copy(req_hbm, req_v.at[o], local_sem.at[0]),
        pltpu.make_async_copy(req_hbm, my_req_s, local_sem.at[1]),
        pltpu.make_async_copy(amp_hbm, mine, local_sem.at[2]),
        pltpu.make_async_copy(int_hbm, ints.at[pl.ds(s * int_local, int_local)], local_sem.at[3]),
        pltpu.make_async_copy(slot_hbm, slot_v.at[r], local_sem.at[4]),
        pltpu.make_async_copy(task_hbm, task_v.at[r], local_sem.at[5]),
        pltpu.make_async_copy(live_hbm, live_v.at[r], local_sem.at[6]),
    ]
    for copy in local:
        copy.start()

    barrier = pltpu.get_barrier_semaphore()
    for d in range(1, owners):
        pl.semaphore_signal(barrier, inc=1, device_id={"owner": lax.rem(o + d, owners)}, device_id_type=MESH)
    for d in range(1, slabs):
        pl.semaphore_signal(barrier, inc=1, device_id={"slab": lax.rem(s + d, slabs)}, device_id_type=MESH)
    for d in range(1, reds):
        pl.semaphore_signal(barrier, inc=1, device_id={"red": lax.rem(r + d, reds)}, device_id_type=MESH)
    dead = slabs * int_local
    ints[dead] = jnp.zeros(ints.shape[1:], ints.dtype)
    for copy in local:
        copy.wait()
    pl.semaphore_wait(barrier, owners - 1 + slabs - 1 + reds - 1)

    def is_near(q):
        return jnp.abs(q - o) == 1

    def is_far(q):
        return jnp.abs(q - o) > 1

    for q in range(owners):
        @pl.when(q != o)
        def _():
            rcopy(req_v.at[o], req_v.at[o], req_send.at[q], req_recv.at[o], owner=q).start()

    def to_neighbours(act):
        @pl.when(o + 1 < owners)
        def _():
            act(rcopy(mine, below, near_send.at[0], near_recv.at[0], owner=jnp.minimum(o + 1, owners - 1)))

        @pl.when(o > 0)
        def _():
            act(rcopy(mine, above, near_send.at[1], near_recv.at[1], owner=jnp.maximum(o - 1, 0)))

    to_neighbours(lambda copy: copy.start())

    def spread(p):
        for dx in range(1, chips):
            there = lax.rem(chip + chips - dx, chips) * CORES + core
            rcopy(own.at[p], far[2 * (dx - 1)].at[p], x_send.at[dx - 1, p], x_recv.at[dx - 1, p], red=there).start()
        rcopy(own.at[p], part.at[p], part_send.at[p], part_recv.at[p], red=mate).start()

    def forward(p):
        for dx in range(1, chips):
            a, b = far[2 * (dx - 1)], far[2 * (dx - 1) + 1]
            rcopy(own.at[p], a.at[p], x_send.at[dx - 1, p], x_recv.at[dx - 1, p], red=mate).wait_recv()
            rcopy(a.at[p], b.at[p], f_send.at[dx - 1, p], f_recv.at[dx - 1, p], red=mate).start()

    own[o] = mine[my_req_s[0, o]]

    half = int_local // CORES
    chunk = half // INT_CHUNKS

    def int_part(slab, which, j):
        return ints.at[pl.ds(slab * int_local + which * half + j * chunk, chunk)]

    for j in range(INT_CHUNKS):
        for d in range(1, slabs):
            rcopy(int_part(s, core, j), int_part(s, core, j), int_send.at[d - 1, j], int_recv.at[d - 1, j],
                  slab=lax.rem(s + d, slabs)).start()

    tables = (slot_v, task_v, live_v)
    for d in range(1, reds):
        for t, ref in enumerate(tables):
            rcopy(ref.at[r], ref.at[r], tab_send.at[d - 1, t], tab_recv.at[d - 1, t],
                  red=lax.rem(r + d, reds)).start()

    for q in range(owners):
        @pl.when(q != o)
        def _():
            rcopy(req_v.at[q], req_v.at[q], req_send.at[q], req_recv.at[q], owner=q).wait_recv()
    to_smem = pltpu.make_async_copy(req_v, req_s, local_sem.at[0])
    to_smem.start()
    spread(o)
    to_smem.wait()
    for q in range(owners):
        @pl.when(is_far(q))
        def _():
            stage[q] = mine[req_s[q, 0, o]]
    for q in range(owners):
        @pl.when(is_far(q))
        def _():
            rcopy(stage.at[q], own.at[o], z_send.at[q], z_recv.at[o], owner=q).start()

    for d in range(1, reds):
        for t, ref in enumerate(tables):
            there = lax.rem(r + reds - d, reds)
            rcopy(ref.at[there], ref.at[there], tab_send.at[d - 1, t], tab_recv.at[d - 1, t], red=there).wait_recv()
    table_copies = [
        pltpu.make_async_copy(ref, to, local_sem.at[1 + t])
        for t, (ref, to) in enumerate(zip(tables, (slot_s, task_s, live_s)))
    ]
    for copy in table_copies:
        copy.start()

    for p in range(owners):
        for side, ref, here in ((0, below, o - 1), (1, above, o + 1)):
            @pl.when(here == p)
            def _():
                rcopy(mine, ref, near_send.at[side], near_recv.at[side], owner=p).wait_recv()
                own[p] = ref[my_req_s[0, p]]
                spread(p)

    forward(o)

    def int_forward(d, j):
        slab = lax.rem(s + slabs - d, slabs)
        rcopy(int_part(slab, core, j), int_part(slab, core, j), int_send.at[d - 1, j], int_recv.at[d - 1, j],
              slab=slab).wait_recv()
        rcopy(int_part(slab, core, j), int_part(slab, core, j), intf_send.at[d - 1, j], intf_recv.at[d - 1, j],
              red=mate).start()

    for j in range(INT_CHUNKS):
        for d in range(1, slabs):
            int_forward(d, j)

    for p in range(owners):
        @pl.when(is_near(p))
        def _():
            forward(p)

    for p in range(owners):
        @pl.when(is_far(p))
        def _():
            rcopy(stage.at[p], own.at[p], z_send.at[p], z_recv.at[p], owner=p).wait_recv()
            spread(p)

    for copy in table_copies:
        copy.wait()
    for j in range(INT_CHUNKS):
        for d in range(1, slabs):
            slab = lax.rem(s + slabs - d, slabs)
            rcopy(int_part(slab, 1 - core, j), int_part(slab, 1 - core, j), intf_send.at[d - 1, j],
                  intf_recv.at[d - 1, j], red=mate).wait_recv()

    def contract(member, tiles, first):
        live = live_s[member, 0, 0]
        for q in range(keep):
            row = r * keep + q
            lhs, rhs = [], []
            for k in range(slots):
                which = jnp.where(k < live, task_s[member, row, k], dead)
                lhs.append(ints[which])
                rhs.append(tiles[slot_s[member, row, k]])
            product = jnp.dot(
                jnp.concatenate(lhs, axis=1), jnp.concatenate(rhs, axis=0), preferred_element_type=jnp.float32
            )
            if first:
                out_ref[q] = product
            else:
                out_ref[q] = out_ref[q] + product

    contract(r, own, True)

    for p in range(owners):
        @pl.when(is_far(p))
        def _():
            forward(p)
    for p in range(owners):
        rcopy(own.at[p], part.at[p], part_send.at[p], part_recv.at[p], red=mate).wait_recv()
    contract(mate, part, False)
    for dx in range(1, chips):
        there = lax.rem(chip + dx, chips)
        contract(there * CORES + core, far[2 * (dx - 1)], False)
        for p in range(owners):
            a, b = far[2 * (dx - 1)], far[2 * (dx - 1) + 1]
            rcopy(a.at[p], b.at[p], f_send.at[dx - 1, p], f_recv.at[dx - 1, p], red=mate).wait_recv()
        contract(there * CORES + (1 - core), far[2 * (dx - 1) + 1], False)

    to_neighbours(lambda copy: copy.wait_send())
    for q in range(owners):
        @pl.when(is_far(q))
        def _():
            rcopy(stage.at[q], own.at[o], z_send.at[q], z_recv.at[o], owner=q).wait_send()

        @pl.when(q != o)
        def _():
            rcopy(req_v.at[o], req_v.at[o], req_send.at[q], req_recv.at[o], owner=q).wait_send()

        for dx in range(1, chips):
            a, b = far[2 * (dx - 1)], far[2 * (dx - 1) + 1]
            rcopy(own.at[q], a.at[q], x_send.at[dx - 1, q], x_recv.at[dx - 1, q], red=mate).wait_send()
            rcopy(a.at[q], b.at[q], f_send.at[dx - 1, q], f_recv.at[dx - 1, q], red=mate).wait_send()
        rcopy(own.at[q], part.at[q], part_send.at[q], part_recv.at[q], red=mate).wait_send()
    for j in range(INT_CHUNKS):
        for d in range(1, slabs):
            to = lax.rem(s + d, slabs)
            frm = lax.rem(s + slabs - d, slabs)
            rcopy(int_part(s, core, j), int_part(s, core, j), int_send.at[d - 1, j], int_recv.at[d - 1, j],
                  slab=to).wait_send()
            rcopy(int_part(frm, core, j), int_part(frm, core, j), intf_send.at[d - 1, j], intf_recv.at[d - 1, j],
                  red=mate).wait_send()
    for d in range(1, reds):
        for t, ref in enumerate(tables):
            rcopy(ref.at[r], ref.at[r], tab_send.at[d - 1, t], tab_recv.at[d - 1, t],
                  red=lax.rem(r + d, reds)).wait_send()


def on_device(sizes, amplitudes, integrals, requests, task_slot, task_integral, live_tasks, denominators):
    owners, slabs, reds = sizes
    per_owner, rows, columns = amplitudes.shape
    int_local, int_rows, int_columns = integrals.shape
    group_tiles, slots = task_slot.shape[3:]
    chips = reds // CORES
    keep = group_tiles // reds
    bf16, i32 = amplitudes.dtype, jnp.int32
    tile_set = pltpu.VMEM((owners, rows, columns), bf16)
    dma = pltpu.SemaphoreType.DMA
    scratch = (
        [
            pltpu.VMEM((per_owner, rows, columns), bf16),
            pltpu.VMEM((slabs * int_local + 1, int_rows, int_columns), bf16),
            pltpu.VMEM((per_owner, rows, columns), bf16),
            pltpu.VMEM((per_owner, rows, columns), bf16),
            tile_set,
            tile_set,
            tile_set,
        ]
        + [tile_set] * (2 * (chips - 1))
        + [
            pltpu.VMEM((owners, 1, owners), i32),
            pltpu.VMEM((reds, group_tiles, slots), i32),
            pltpu.VMEM((reds, group_tiles, slots), i32),
            pltpu.VMEM((reds, 1, 1), i32),
            pltpu.SMEM((1, owners), i32),
            pltpu.SMEM((owners, 1, owners), i32),
            pltpu.SMEM((reds, group_tiles, slots), i32),
            pltpu.SMEM((reds, group_tiles, slots), i32),
            pltpu.SMEM((reds, 1, 1), i32),
            dma((7,)),
            dma((owners,)), dma((owners,)),
            dma((reds - 1, 3)), dma((reds - 1, 3)),
            dma((2,)), dma((2,)),
            dma((owners,)), dma((owners,)),
            dma((slabs - 1, INT_CHUNKS)), dma((slabs - 1, INT_CHUNKS)),
            dma((slabs - 1, INT_CHUNKS)), dma((slabs - 1, INT_CHUNKS)),
            dma((owners,)), dma((owners,)),
            dma((chips - 1, owners)), dma((chips - 1, owners)),
            dma((chips - 1, owners)), dma((chips - 1, owners)),
        ]
    )
    whole = (owners, slabs, reds, per_owner, int_local, group_tiles, slots)
    residual = pl.pallas_call(
        functools.partial(kernel, whole),
        out_shape=jax.ShapeDtypeStruct((keep, rows, columns), jnp.float32),
        in_specs=[pl.BlockSpec(memory_space=pl.ANY)] * 6,
        out_specs=pl.BlockSpec(memory_space=pltpu.VMEM),
        scratch_shapes=scratch,
        compiler_params=pltpu.CompilerParams(collective_id=0, has_side_effects=True),
        name="gather_contract",
    )(
        amplitudes,
        integrals,
        requests.reshape(1, owners),
        task_slot.reshape(group_tiles, slots),
        task_integral.reshape(group_tiles, slots),
        live_tasks.reshape(1, 1),
    )
    return residual / denominators


def solution(mesh):
    placed = (
        P(("owner", "slab", "red"), None, None),
        P("slab", None, None),
        P("owner", "slab", "red", None),
        P("owner", "slab", "red", None, None),
        P("owner", "slab", "red", None, None),
        P("owner", "slab", "red"),
        P(("owner", "slab", "red"), None, None),
    )
    sizes = (mesh.shape["owner"], mesh.shape["slab"], mesh.shape["red"])
    return jax.shard_map(
        functools.partial(on_device, sizes),
        mesh=mesh,
        in_specs=placed,
        out_specs=P(("owner", "slab", "red"), None, None),
        check_vma=False,
    )
```

```python
import functools

import jax
import jax.numpy as jnp
from jax import lax
from jax.experimental import pallas as pl
from jax.experimental.pallas import tpu as pltpu
from jax.sharding import PartitionSpec as P

MESH = pl.DeviceIdType.MESH
CORES = 2
INT_CHUNKS = 2


def kernel(sizes, amp_hbm, int_hbm, req_hbm, slot_hbm, task_hbm, live_hbm, out_ref, *scratch):
    owners, slabs, reds, per_owner, int_local, group_tiles, slots = sizes
    chips = reds // CORES
    keep = group_tiles // reds
    (mine, ints, below, above, stage, own, part) = scratch[:7]
    far = scratch[7 : 7 + 2 * (chips - 1)]
    (req_v, slot_v, task_v, live_v, my_req_s, req_s, slot_s, task_s, live_s,
     local_sem, req_send, req_recv, tab_send, tab_recv, near_send, near_recv, z_send, z_recv,
     int_send, int_recv, intf_send, intf_recv, part_send, part_recv,
     x_send, x_recv, f_send, f_recv) = scratch[7 + 2 * (chips - 1):]
    o = lax.axis_index("owner")
    s = lax.axis_index("slab")
    r = lax.axis_index("red")
    chip = r // CORES
    core = r % CORES
    mate = chip * CORES + (1 - core)

    def rcopy(src, dst, send, recv, **where):
        return pltpu.make_async_remote_copy(
            src_ref=src, dst_ref=dst, send_sem=send, recv_sem=recv, device_id=where, device_id_type=MESH
        )

    local = [
        pltpu.make_async_copy(req_hbm, req_v.at[o], local_sem.at[0]),
        pltpu.make_async_copy(req_hbm, my_req_s, local_sem.at[1]),
        pltpu.make_async_copy(amp_hbm, mine, local_sem.at[2]),
        pltpu.make_async_copy(int_hbm, ints.at[pl.ds(s * int_local, int_local)], local_sem.at[3]),
        pltpu.make_async_copy(slot_hbm, slot_v.at[r], local_sem.at[4]),
        pltpu.make_async_copy(task_hbm, task_v.at[r], local_sem.at[5]),
        pltpu.make_async_copy(live_hbm, live_v.at[r], local_sem.at[6]),
    ]
    for copy in local:
        copy.start()

    barrier = pltpu.get_barrier_semaphore()
    for d in range(1, owners):
        pl.semaphore_signal(barrier, inc=1, device_id={"owner": lax.rem(o + d, owners)}, device_id_type=MESH)
    for d in range(1, slabs):
        pl.semaphore_signal(barrier, inc=1, device_id={"slab": lax.rem(s + d, slabs)}, device_id_type=MESH)
    for d in range(1, reds):
        pl.semaphore_signal(barrier, inc=1, device_id={"red": lax.rem(r + d, reds)}, device_id_type=MESH)
    dead = slabs * int_local
    ints[dead] = jnp.zeros(ints.shape[1:], ints.dtype)
    for copy in local:
        copy.wait()
    pl.semaphore_wait(barrier, owners - 1 + slabs - 1 + reds - 1)

    def is_near(q):
        return jnp.abs(q - o) == 1

    def each_far(act, nearest_first=True):
        distances = range(2, owners)
        for d in distances if nearest_first else reversed(distances):
            for q, inside in ((o - d, o >= d), (o + d, o + d < owners)):
                q = jnp.clip(q, 0, owners - 1)
                pl.when(inside)(functools.partial(act, q))

    for q in range(owners):
        @pl.when(q != o)
        def _():
            rcopy(req_v.at[o], req_v.at[o], req_send.at[q], req_recv.at[o], owner=q).start()

    def to_neighbours(act):
        @pl.when(o + 1 < owners)
        def _():
            act(rcopy(mine, below, near_send.at[0], near_recv.at[0], owner=jnp.minimum(o + 1, owners - 1)))

        @pl.when(o > 0)
        def _():
            act(rcopy(mine, above, near_send.at[1], near_recv.at[1], owner=jnp.maximum(o - 1, 0)))

    to_neighbours(lambda copy: copy.start())

    def spread(p):
        for dx in range(1, chips):
            there = lax.rem(chip + chips - dx, chips) * CORES + core
            rcopy(own.at[p], far[2 * (dx - 1)].at[p], x_send.at[dx - 1, p], x_recv.at[dx - 1, p], red=there).start()
        rcopy(own.at[p], part.at[p], part_send.at[p], part_recv.at[p], red=mate).start()

    def forward(p):
        for dx in range(1, chips):
            a, b = far[2 * (dx - 1)], far[2 * (dx - 1) + 1]
            rcopy(own.at[p], a.at[p], x_send.at[dx - 1, p], x_recv.at[dx - 1, p], red=mate).wait_recv()
            rcopy(a.at[p], b.at[p], f_send.at[dx - 1, p], f_recv.at[dx - 1, p], red=mate).start()

    own[o] = mine[my_req_s[0, o]]

    half = int_local // CORES
    chunk = half // INT_CHUNKS

    def int_part(slab, which, j):
        return ints.at[pl.ds(slab * int_local + which * half + j * chunk, chunk)]

    for j in range(INT_CHUNKS):
        for d in range(1, slabs):
            rcopy(int_part(s, core, j), int_part(s, core, j), int_send.at[d - 1, j], int_recv.at[d - 1, j],
                  slab=lax.rem(s + d, slabs)).start()

    tables = (slot_v, task_v, live_v)
    for d in range(1, reds):
        for t, ref in enumerate(tables):
            rcopy(ref.at[r], ref.at[r], tab_send.at[d - 1, t], tab_recv.at[d - 1, t],
                  red=lax.rem(r + d, reds)).start()

    for q in range(owners):
        @pl.when(q != o)
        def _():
            rcopy(req_v.at[q], req_v.at[q], req_send.at[q], req_recv.at[q], owner=q).wait_recv()
    to_smem = pltpu.make_async_copy(req_v, req_s, local_sem.at[0])
    to_smem.start()
    spread(o)
    to_smem.wait()
    def select(q):
        stage[q] = mine[req_s[q, 0, o]]

    each_far(select, nearest_first=False)
    each_far(lambda q: rcopy(stage.at[q], own.at[o], z_send.at[q], z_recv.at[o], owner=q).start(), nearest_first=False)

    for d in range(1, reds):
        for t, ref in enumerate(tables):
            there = lax.rem(r + reds - d, reds)
            rcopy(ref.at[there], ref.at[there], tab_send.at[d - 1, t], tab_recv.at[d - 1, t], red=there).wait_recv()
    table_copies = [
        pltpu.make_async_copy(ref, to, local_sem.at[1 + t])
        for t, (ref, to) in enumerate(zip(tables, (slot_s, task_s, live_s)))
    ]
    for copy in table_copies:
        copy.start()

    for p in range(owners):
        for side, ref, here in ((0, below, o - 1), (1, above, o + 1)):
            @pl.when(here == p)
            def _():
                rcopy(mine, ref, near_send.at[side], near_recv.at[side], owner=p).wait_recv()
                own[p] = ref[my_req_s[0, p]]
                spread(p)

    forward(o)

    def int_forward(d, j):
        slab = lax.rem(s + slabs - d, slabs)
        rcopy(int_part(slab, core, j), int_part(slab, core, j), int_send.at[d - 1, j], int_recv.at[d - 1, j],
              slab=slab).wait_recv()
        rcopy(int_part(slab, core, j), int_part(slab, core, j), intf_send.at[d - 1, j], intf_recv.at[d - 1, j],
              red=mate).start()

    for j in range(INT_CHUNKS):
        for d in range(1, slabs):
            int_forward(d, j)

    for p in range(owners):
        @pl.when(is_near(p))
        def _():
            forward(p)

    def pulled_far(p):
        rcopy(stage.at[p], own.at[p], z_send.at[p], z_recv.at[p], owner=p).wait_recv()
        spread(p)

    each_far(pulled_far)

    for copy in table_copies:
        copy.wait()
    for j in range(INT_CHUNKS):
        for d in range(1, slabs):
            slab = lax.rem(s + slabs - d, slabs)
            rcopy(int_part(slab, 1 - core, j), int_part(slab, 1 - core, j), intf_send.at[d - 1, j],
                  intf_recv.at[d - 1, j], red=mate).wait_recv()

    def contract(member, tiles, first):
        live = live_s[member, 0, 0]
        for q in range(keep):
            row = r * keep + q
            lhs, rhs = [], []
            for k in range(slots):
                which = jnp.where(k < live, task_s[member, row, k], dead)
                lhs.append(ints[which])
                rhs.append(tiles[slot_s[member, row, k]])
            product = jnp.dot(
                jnp.concatenate(lhs, axis=1), jnp.concatenate(rhs, axis=0), preferred_element_type=jnp.float32
            )
            if first:
                out_ref[q] = product
            else:
                out_ref[q] = out_ref[q] + product

    contract(r, own, True)

    each_far(forward)
    for p in range(owners):
        rcopy(own.at[p], part.at[p], part_send.at[p], part_recv.at[p], red=mate).wait_recv()
    contract(mate, part, False)
    for dx in range(1, chips):
        there = lax.rem(chip + dx, chips)
        contract(there * CORES + core, far[2 * (dx - 1)], False)
        for p in range(owners):
            a, b = far[2 * (dx - 1)], far[2 * (dx - 1) + 1]
            rcopy(a.at[p], b.at[p], f_send.at[dx - 1, p], f_recv.at[dx - 1, p], red=mate).wait_recv()
        contract(there * CORES + (1 - core), far[2 * (dx - 1) + 1], False)

    to_neighbours(lambda copy: copy.wait_send())
    each_far(lambda q: rcopy(stage.at[q], own.at[o], z_send.at[q], z_recv.at[o], owner=q).wait_send())
    for q in range(owners):
        @pl.when(q != o)
        def _():
            rcopy(req_v.at[o], req_v.at[o], req_send.at[q], req_recv.at[o], owner=q).wait_send()

        for dx in range(1, chips):
            a, b = far[2 * (dx - 1)], far[2 * (dx - 1) + 1]
            rcopy(own.at[q], a.at[q], x_send.at[dx - 1, q], x_recv.at[dx - 1, q], red=mate).wait_send()
            rcopy(a.at[q], b.at[q], f_send.at[dx - 1, q], f_recv.at[dx - 1, q], red=mate).wait_send()
        rcopy(own.at[q], part.at[q], part_send.at[q], part_recv.at[q], red=mate).wait_send()
    for j in range(INT_CHUNKS):
        for d in range(1, slabs):
            to = lax.rem(s + d, slabs)
            frm = lax.rem(s + slabs - d, slabs)
            rcopy(int_part(s, core, j), int_part(s, core, j), int_send.at[d - 1, j], int_recv.at[d - 1, j],
                  slab=to).wait_send()
            rcopy(int_part(frm, core, j), int_part(frm, core, j), intf_send.at[d - 1, j], intf_recv.at[d - 1, j],
                  red=mate).wait_send()
    for d in range(1, reds):
        for t, ref in enumerate(tables):
            rcopy(ref.at[r], ref.at[r], tab_send.at[d - 1, t], tab_recv.at[d - 1, t],
                  red=lax.rem(r + d, reds)).wait_send()


def on_device(sizes, amplitudes, integrals, requests, task_slot, task_integral, live_tasks, denominators):
    owners, slabs, reds = sizes
    per_owner, rows, columns = amplitudes.shape
    int_local, int_rows, int_columns = integrals.shape
    group_tiles, slots = task_slot.shape[3:]
    chips = reds // CORES
    keep = group_tiles // reds
    bf16, i32 = amplitudes.dtype, jnp.int32
    tile_set = pltpu.VMEM((owners, rows, columns), bf16)
    dma = pltpu.SemaphoreType.DMA
    scratch = (
        [
            pltpu.VMEM((per_owner, rows, columns), bf16),
            pltpu.VMEM((slabs * int_local + 1, int_rows, int_columns), bf16),
            pltpu.VMEM((per_owner, rows, columns), bf16),
            pltpu.VMEM((per_owner, rows, columns), bf16),
            tile_set,
            tile_set,
            tile_set,
        ]
        + [tile_set] * (2 * (chips - 1))
        + [
            pltpu.VMEM((owners, 1, owners), i32),
            pltpu.VMEM((reds, group_tiles, slots), i32),
            pltpu.VMEM((reds, group_tiles, slots), i32),
            pltpu.VMEM((reds, 1, 1), i32),
            pltpu.SMEM((1, owners), i32),
            pltpu.SMEM((owners, 1, owners), i32),
            pltpu.SMEM((reds, group_tiles, slots), i32),
            pltpu.SMEM((reds, group_tiles, slots), i32),
            pltpu.SMEM((reds, 1, 1), i32),
            dma((7,)),
            dma((owners,)), dma((owners,)),
            dma((reds - 1, 3)), dma((reds - 1, 3)),
            dma((2,)), dma((2,)),
            dma((owners,)), dma((owners,)),
            dma((slabs - 1, INT_CHUNKS)), dma((slabs - 1, INT_CHUNKS)),
            dma((slabs - 1, INT_CHUNKS)), dma((slabs - 1, INT_CHUNKS)),
            dma((owners,)), dma((owners,)),
            dma((chips - 1, owners)), dma((chips - 1, owners)),
            dma((chips - 1, owners)), dma((chips - 1, owners)),
        ]
    )
    whole = (owners, slabs, reds, per_owner, int_local, group_tiles, slots)
    residual = pl.pallas_call(
        functools.partial(kernel, whole),
        out_shape=jax.ShapeDtypeStruct((keep, rows, columns), jnp.float32),
        in_specs=[pl.BlockSpec(memory_space=pl.ANY)] * 6,
        out_specs=pl.BlockSpec(memory_space=pltpu.VMEM),
        scratch_shapes=scratch,
        compiler_params=pltpu.CompilerParams(collective_id=0, has_side_effects=True),
        name="gather_contract",
    )(
        amplitudes,
        integrals,
        requests.reshape(1, owners),
        task_slot.reshape(group_tiles, slots),
        task_integral.reshape(group_tiles, slots),
        live_tasks.reshape(1, 1),
    )
    return residual / denominators


def solution(mesh):
    placed = (
        P(("owner", "slab", "red"), None, None),
        P("slab", None, None),
        P("owner", "slab", "red", None),
        P("owner", "slab", "red", None, None),
        P("owner", "slab", "red", None, None),
        P("owner", "slab", "red"),
        P(("owner", "slab", "red"), None, None),
    )
    sizes = (mesh.shape["owner"], mesh.shape["slab"], mesh.shape["red"])
    return jax.shard_map(
        functools.partial(on_device, sizes),
        mesh=mesh,
        in_specs=placed,
        out_specs=P(("owner", "slab", "red"), None, None),
        check_vma=False,
    )
```
